32 devices in a mesh: tok: 16 (over z, y, core), cand: 2 (over x).
Axes of the slice: x: 2, y: 2, z: 4, core: 2. Of those that a mesh axis runs over, the one named last changes fastest.
Arguments:
- dec_hidden: bfloat16 [2, 16, 32, 2048], P(None, 'cand'), may hold values from -6 to 6
- enc_keys: bfloat16 [2, 2048, 2048], P(None, 'tok'), may hold values from -250 to 250
- enc_values: bfloat16 [2, 2048, 2048], P(None, 'tok'), may hold values from -72 to 72
- enc_lengths: int32 [2], replicated, may hold values from 512 to 2048, as said below
- cand_counts: int32 [2], replicated, may hold values from 4 to 16, as said below
- gold_ids: int32 [2, 16, 32], P(None, 'cand'), may hold values from 0 to 32127
- gain_cross: float32 [2048], replicated, may hold values from 0.25 to 1.75
- w_query: bfloat16 [2048, 2048], P('cand', 'tok'), may hold values from -0.125 to 0.125
- w_out: bfloat16 [2048, 2048], P('tok', 'cand'), may hold values from -0.125 to 0.125
- gain_ffn: float32 [2048], replicated, may hold values from 0.25 to 1.75
- w_in_gate: bfloat16 [2048, 5120], P('cand', 'tok'), may hold values from -0.125 to 0.125
- w_in_up: bfloat16 [2048, 5120], P('cand', 'tok'), may hold values from -0.125 to 0.125
- w_ffn_out: bfloat16 [5120, 2048], P('tok', 'cand'), may hold values from -0.25 to 0.25
- gain_final: float32 [2048], replicated, may hold values from 0.25 to 1.75
- w_vocab: bfloat16 [2048, 32128], P('cand', 'tok'), may hold values from -20 to 20
Outputs:
- cand_scores: float32 [2, 16], P(None, 'cand')
- best_score: float32 [2], replicated
The draws below stay inside these ranges and needn't reach their ends.
Inputs may be any that keep to these rules, and one draw needn't show every extreme that they name: `enc_lengths`: some query has all 2048 encoder tokens live. `cand_counts`: some query has all 16 candidates live.
All inputs are finite; a program needn't handle non-finite values.
Results may differ from the reference program's by a relative error of at most 0.0014.
The reference program's roundings to bfloat16 on the way count: a program that leaves them out, or rounds other values in their place, can miss the bound.
Values may be sent and summed in bfloat16 or wider, within the bound.
A program may use at most 64 MiB of HBM per device.

```python
import math
import jax
import jax.numpy as jnp
import numpy as np
from jax import lax

D = 2048
HEADS = 32
HEAD_DIM = 64
FF = 5120
VOCAB = 32128
QUERIES = 2
LENGTH = 32
CANDS = 16
SRC = 2048


def draw_enc_keys(key, part):
    base = 0.25 * jax.random.truncated_normal(key, -6.0, 6.0, (QUERIES, SRC, D), jnp.float32)
    return base.astype(jnp.bfloat16)


def draw_w_vocab(key, part):
    base = 4.0 * jax.random.truncated_normal(key, -6.0, 6.0, (D, VOCAB), jnp.float32) / jnp.sqrt(float(D))
    return jnp.clip(base, -20.0, 20.0).astype(jnp.bfloat16)


def draw_enc_lengths(key, part):
    drawn = jax.random.randint(key, (QUERIES,), SRC // 4, SRC + 1)
    chosen = jax.random.randint(jax.random.fold_in(key, 7), (), 0, QUERIES)
    return jnp.where(jnp.arange(QUERIES) == chosen, SRC, drawn).astype(jnp.int32)


def draw_cand_counts(key, part):
    drawn = jax.random.randint(key, (QUERIES,), CANDS // 4, CANDS + 1)
    chosen = jax.random.randint(jax.random.fold_in(key, 11), (), 0, QUERIES)
    return jnp.where(jnp.arange(QUERIES) == chosen, CANDS, drawn).astype(jnp.int32)


def set_ends(values, stream_key, smallest, largest):
    place = [jax.random.randint(jax.random.fold_in(stream_key, axis), (), 0, length) for axis, length in enumerate(values.shape)]
    longest = values.shape.index(max(values.shape))
    beside = place[:longest] + [(place[longest] + 1) % values.shape[longest]] + place[longest + 1:]
    return values.at[tuple(place)].set(smallest).at[tuple(beside)].set(largest)


def block_levels(own_key, dims, split, smallest, top_value):
    level, own = 1.0, jax.random.fold_in(own_key, 6)
    for axis_at, blocks in split:
        heights = jnp.exp(jax.random.uniform(jax.random.fold_in(own, axis_at), (blocks,), jnp.float32, smallest / len(split), top_value / len(split)))
        level = level * jnp.repeat(heights, dims[axis_at] // blocks).reshape([-1 if axis == axis_at else 1 for axis in range(len(dims))])
    return level


def rank_table(count, skew):
    portions = [(1 << 20) // math.isqrt(rank ** skew) + 1 for rank in range(1, count + 1)]
    width = 1 + sum(portions) // (1 << 30)
    return np.cumsum(np.array([max(1, weight // width) for weight in portions]))


def ranked(own_key, shape, number_of, slope):
    grid = rank_table(number_of, slope)
    lot = jax.random.randint(jax.random.fold_in(own_key, 1), shape, 0, int(grid[number_of - 1]))
    grade = jnp.searchsorted(jnp.asarray(grid, jnp.int32), lot, side="right")
    return jax.random.permutation(jax.random.fold_in(own_key, 2), number_of)[grade].astype(jnp.int32)


def centred(stream_key, extent, deviation, limit, shards=(), kind=jnp.bfloat16):
    values = jax.random.normal(stream_key, extent, jnp.float32) * deviation
    if len(shards) > 0:
        values = block_levels(stream_key, extent, shards, -0.22, 0.18) * values
    return jnp.clip(values, min=-limit, max=limit).astype(kind)


def setup_inputs(seed: int = 0) -> dict:
    keys = jax.random.split(jax.random.key(seed), 16)
    return {
        "dec_hidden": centred(keys[0], (QUERIES, CANDS, LENGTH, D), 1.0, 6.0, ((1, 2),)),
        "enc_keys": draw_enc_keys(jax.random.fold_in(keys[15], 71), 0),
        "enc_values": centred(keys[2], (QUERIES, SRC, D), 12.0, 72.0, ((1, 16),)),
        "enc_lengths": draw_enc_lengths(jax.random.fold_in(keys[15], 71), 0),
        "cand_counts": draw_cand_counts(jax.random.fold_in(keys[15], 71), 0),
        "gold_ids": set_ends(ranked(keys[5], (QUERIES, CANDS, LENGTH), VOCAB, 2), jax.random.fold_in(keys[5], 3), 0, VOCAB - 1).astype(jnp.int32),
        "gain_cross": jnp.clip(1.0 + 0.15 * jax.random.normal(keys[6], (D,), jnp.float32), 0.25, 1.75),
        "w_query": centred(keys[7], (D, D), D ** -0.5, 0.125, ((0, 2), (1, 16))),
        "w_out": centred(keys[8], (D, D), D ** -0.5, 0.125, ((0, 16), (1, 2))),
        "gain_ffn": jnp.clip(1.0 + 0.15 * jax.random.normal(keys[9], (D,), jnp.float32), 0.25, 1.75),
        "w_in_gate": centred(keys[10], (D, FF), D ** -0.5, 0.125, ((0, 2), (1, 16))),
        "w_in_up": centred(keys[11], (D, FF), D ** -0.5, 0.125, ((0, 2), (1, 16))),
        "w_ffn_out": centred(keys[12], (FF, D), (FF // 9) ** -0.5, 0.25, ((0, 16), (1, 2))),
        "gain_final": jnp.clip(1.0 + 0.15 * jax.random.normal(keys[13], (D,), jnp.float32), 0.25, 1.75),
        "w_vocab": draw_w_vocab(jax.random.fold_in(keys[15], 71), 0),
    }


norm_eps = 0.25

def root_norm(values, gain):
    squares = lax.optimization_barrier(jnp.mean(values * values, axis=-1, keepdims=True))
    return values * lax.rsqrt(squares + norm_eps) * gain

def reference(dec_hidden, enc_keys, enc_values, enc_lengths, cand_counts, gold_ids, gain_cross, w_query, w_out, gain_ffn, w_in_gate, w_in_up, w_ffn_out, gain_final, w_vocab):
    total_rows = QUERIES * CANDS * LENGTH
    inputs_flat = dec_hidden.reshape(total_rows, D).astype(jnp.float32)
    normed = root_norm(inputs_flat, gain_cross).astype(jnp.bfloat16)
    queries_all = jnp.dot(normed, w_query, preferred_element_type=jnp.float32).astype(jnp.bfloat16)
    queries_all = lax.optimization_barrier(queries_all)
    query_heads = queries_all.reshape(QUERIES, CANDS * LENGTH, HEADS, HEAD_DIM).transpose(2, 0, 1, 3).astype(jnp.float32)
    key_heads = enc_keys.reshape(QUERIES, SRC, HEADS, HEAD_DIM).transpose(2, 0, 1, 3).astype(jnp.float32)
    value_heads = enc_values.reshape(QUERIES, SRC, HEADS, HEAD_DIM).transpose(2, 0, 1, 3).astype(jnp.float32)
    live_keys = jnp.arange(SRC, dtype=jnp.int32)[None, :] < enc_lengths[:, None]

    def attend(operands):
        query_head, key_head, value_head = operands
        scores = jnp.einsum('brd,bsd->brs', query_head, key_head, precision=lax.Precision.HIGHEST)
        scores = jnp.where(live_keys[:, None, :], scores, -1e+30)
        row_max = lax.optimization_barrier(jnp.max(scores, axis=-1, keepdims=True))
        weights = jnp.where(live_keys[:, None, :], jnp.exp(scores - row_max), 0.0)
        denominator = lax.optimization_barrier(jnp.sum(weights, axis=-1, keepdims=True))
        rounded = lax.optimization_barrier(weights.astype(jnp.bfloat16)).astype(jnp.float32)
        mixed_values = jnp.einsum('brs,bsd->brd', rounded, value_head, precision=lax.Precision.HIGHEST)
        return (mixed_values / denominator).astype(jnp.bfloat16)
    attended = lax.map(attend, (query_heads, key_heads, value_heads))
    attended = attended.transpose(1, 2, 0, 3).reshape(total_rows, D)
    after_cross = inputs_flat + jnp.dot(attended, w_out, preferred_element_type=jnp.float32)
    normed_ffn = root_norm(after_cross, gain_ffn).astype(jnp.bfloat16)
    gate_part = jnp.dot(normed_ffn, w_in_gate, preferred_element_type=jnp.float32)
    up_part = jnp.dot(normed_ffn, w_in_up, preferred_element_type=jnp.float32)
    hidden = (jax.nn.gelu(gate_part, approximate=True) * up_part).astype(jnp.bfloat16)
    after_ffn = after_cross + jnp.dot(hidden, w_ffn_out, preferred_element_type=jnp.float32)
    normed_final = root_norm(after_ffn, gain_final).astype(jnp.bfloat16)
    block_rows = 512 if total_rows % 512 == 0 else total_rows

    def score_block(operands):
        rows_block, gold_block = operands
        logits = jnp.dot(rows_block, w_vocab, preferred_element_type=jnp.float32)
        row_max = lax.optimization_barrier(jnp.max(logits, axis=1))
        sum_exp = lax.optimization_barrier(jnp.sum(jnp.exp(logits - row_max[:, None]), axis=1))
        picked = jnp.take_along_axis(logits, gold_block[:, None], axis=1)[:, 0]
        return picked - row_max - jnp.log(sum_exp)
    logprob = lax.map(score_block, (normed_final.reshape(-1, block_rows, D), gold_ids.reshape(-1, block_rows)))
    per_cand = lax.optimization_barrier(jnp.mean(logprob.reshape(QUERIES, CANDS, LENGTH), axis=2))
    valid_cand = jnp.arange(CANDS, dtype=jnp.int32)[None, :] < cand_counts[:, None]
    cand_scores = jnp.where(valid_cand, per_cand, 0.0)
    best_score = lax.optimization_barrier(jnp.max(jnp.where(valid_cand, per_cand, -1e+30), axis=1))
    return (cand_scores, best_score)
```

```python
import functools

import jax
import jax.numpy as jnp
from jax import lax
from jax.experimental import pallas as pl
from jax.experimental.pallas import tpu as pltpu
from jax.sharding import PartitionSpec as P

HEAD_DIM = 64
MESH = pl.DeviceIdType.MESH

norm_eps = 0.25
BF = jnp.bfloat16
F32 = jnp.float32


def root_norm(values, gain):
    squares = jnp.mean(values * values, axis=-1, keepdims=True)
    return values * lax.rsqrt(squares + norm_eps) * gain


def dot32(left_side, piece):
    return jnp.dot(left_side, piece, preferred_element_type=F32)


def mix_kernel(n, pieces, sub, *refs):
    part = refs[:pieces]
    resid, gain = refs[pieces : pieces + 2]
    after, every = refs[pieces + 2 : pieces + 4]
    (
        send_c, recv_c, send_y, recv_y, send_z, recv_z,
        cs, cr, ys, yr, zs, zr, gzs, gzr, gys, gyr, gcs, gcr,
    ) = refs[pieces + 4 :]
    outer = n // 4
    width = send_c.shape[-1]
    chunks = pieces * sub
    me = lax.axis_index("tok")
    a, y, c = me // 4, (me // 2) % 2, me % 2
    core_peer = a * 4 + y * 2 + (1 - c)
    mid_peer = a * 4 + (1 - y) * 2 + c

    def outer_peer(k):
        return ((a + k) % outer) * 4 + y * 2 + c

    barrier = pltpu.get_barrier_semaphore()
    peers = [core_peer, mid_peer] + [outer_peer(k) for k in range(1, outer)]
    for peer in peers:
        pl.semaphore_signal(barrier, inc=1, device_id={"tok": peer}, device_id_type=MESH)

    def remote(src, dst, s, r, peer):
        return pltpu.make_async_remote_copy(
            src_ref=src, dst_ref=dst, send_sem=s, recv_sem=r,
            device_id={"tok": peer}, device_id_type=MESH,
        )

    def piece_of(ch):
        at = (ch % sub) * width
        return part[ch // sub], slice(at, at + width)

    copies = []
    for ch in range(chunks):
        ref, cols = piece_of(ch)
        for i in range(outer):
            for m in range(2):
                send_c[ch, i * 2 + m] = ref[i * 4 + m * 2 + (1 - c), :, cols].astype(BF)
        if ch == 0:
            pl.semaphore_wait(barrier, len(peers))
        cp = remote(send_c.at[ch], recv_c.at[ch], cs.at[ch], cr.at[ch], core_peer)
        cp.start()
        copies.append(cp)
    core_copies = list(copies)
    mid_copies = []
    for ch in range(chunks):
        ref, cols = piece_of(ch)
        core_copies[ch].wait_recv()
        for i in range(outer):
            other = 1 - y
            send_y[ch, i] = (
                ref[i * 4 + other * 2 + c, :, cols] + recv_c[ch, i * 2 + other].astype(F32)
            ).astype(BF)
        cp = remote(send_y.at[ch], recv_y.at[ch], ys.at[ch], yr.at[ch], mid_peer)
        cp.start()
        copies.append(cp)
        mid_copies.append(cp)

    def joined(ch, i):
        ref, cols = piece_of(ch)
        return (
            ref[i * 4 + y * 2 + c, :, cols]
            + recv_c[ch, i * 2 + y].astype(F32)
            + recv_y[ch, i].astype(F32)
        )

    outer_copies = []
    for ch in range(chunks):
        mid_copies[ch].wait_recv()
        row = []
        for k in range(1, outer):
            to = (a + k) % outer
            send_z[ch, k - 1] = joined(ch, to).astype(BF)
            cp = remote(
                send_z.at[ch, k - 1], recv_z.at[ch, k - 1],
                zs.at[ch, k - 1], zr.at[ch, k - 1], outer_peer(k),
            )
            cp.start()
            copies.append(cp)
            row.append(cp)
        outer_copies.append(row)
    for ch in range(chunks):
        total = joined(ch, a)
        for k in range(1, outer):
            outer_copies[ch][k - 1].wait_recv()
            total = total + recv_z[ch, k - 1].astype(F32)
        cols = slice(ch * width, (ch + 1) * width)
        after[:, cols] = resid[:, cols] + total
    values = after[...]
    every[me] = root_norm(values, gain[...]).astype(BF)

    gz, gy, gc = [], [], []
    for k in range(1, outer):
        cp = remote(every.at[me], every.at[me], gzs.at[k - 1], gzr.at[k - 1], outer_peer(k))
        cp.start()
        gz.append(cp)

    def block(k, m, e):
        return ((a + outer - k) % outer) * 4 + m * 2 + e

    def to_mid(k):
        b = block(k, y, c)
        cp = remote(every.at[b], every.at[b], gys.at[k], gyr.at[k], mid_peer)
        cp.start()
        gy.append(cp)

    def to_core(k, m, slot):
        b = block(k, m, c)
        cp = remote(every.at[b], every.at[b], gcs.at[slot], gcr.at[slot], core_peer)
        cp.start()
        gc.append(cp)

    to_mid(0)
    to_core(0, y, 0)
    for k in range(1, outer):
        gz[k - 1].wait_recv()
        to_mid(k)
        to_core(k, y, 2 * k)
    for k in range(outer):
        gy[k].wait_recv()
        to_core(k, 1 - y, 2 * k + 1)
    for cp in gc:
        cp.wait_recv()
    for cp in copies + gz + gy + gc:
        cp.wait_send()


def mix(parts, resid, gain, n, ident):
    pieces = len(parts)
    share, width = resid.shape
    sub = max(1, 4 // pieces)
    cw = width // pieces // sub
    chunks = pieces * sub
    outer = n // 4
    vm = pl.BlockSpec(memory_space=pltpu.VMEM)
    dma = pltpu.SemaphoreType.DMA
    parts = [p.reshape(n, share, width // pieces) for p in parts]
    return pl.pallas_call(
        functools.partial(mix_kernel, n, pieces, sub),
        out_shape=(
            jax.ShapeDtypeStruct((share, width), F32),
            jax.ShapeDtypeStruct((n, share, width), BF),
        ),
        in_specs=[vm] * (pieces + 2),
        out_specs=(vm, vm),
        scratch_shapes=[
            pltpu.VMEM((chunks, outer * 2, share, cw), BF),
            pltpu.VMEM((chunks, outer * 2, share, cw), BF),
            pltpu.VMEM((chunks, outer, share, cw), BF),
            pltpu.VMEM((chunks, outer, share, cw), BF),
            pltpu.VMEM((chunks, outer - 1, share, cw), BF),
            pltpu.VMEM((chunks, outer - 1, share, cw), BF),
            dma((chunks,)), dma((chunks,)), dma((chunks,)), dma((chunks,)),
            dma((chunks, outer - 1)), dma((chunks, outer - 1)),
            dma((outer - 1,)), dma((outer - 1,)),
            dma((outer,)), dma((outer,)), dma((2 * outer,)), dma((2 * outer,)),
        ],
        compiler_params=pltpu.CompilerParams(
            collective_id=ident, has_side_effects=True, vmem_limit_bytes=32 << 20
        ),
        cost_estimate=pl.CostEstimate(
            flops=10**7, bytes_accessed=100 * 10**6, transcendentals=0
        ),
        name=f"mix{ident}",
    )(*parts, resid, gain.reshape(1, width))


def stats_kernel(n, mine, out, ss, rs):
    me = lax.axis_index("tok")
    barrier = pltpu.get_barrier_semaphore()
    for k in range(1, n):
        pl.semaphore_signal(
            barrier, inc=1, device_id={"tok": (me + k) % n}, device_id_type=MESH
        )
    out[me] = mine[...]
    pl.semaphore_wait(barrier, n - 1)
    copies = []
    for k in range(1, n):
        cp = pltpu.make_async_remote_copy(
            src_ref=mine, dst_ref=out.at[me], send_sem=ss.at[k - 1], recv_sem=rs.at[k - 1],
            device_id={"tok": (me + k) % n}, device_id_type=MESH,
        )
        cp.start()
        copies.append(cp)
    for cp in copies:
        cp.wait_recv()
    for cp in copies:
        cp.wait_send()


def gather_stats(mine, n):
    vm = pl.BlockSpec(memory_space=pltpu.VMEM)
    return pl.pallas_call(
        functools.partial(stats_kernel, n),
        out_shape=jax.ShapeDtypeStruct((n,) + mine.shape, F32),
        in_specs=[vm],
        out_specs=vm,
        scratch_shapes=[pltpu.SemaphoreType.DMA((n - 1,)), pltpu.SemaphoreType.DMA((n - 1,))],
        compiler_params=pltpu.CompilerParams(collective_id=3, has_side_effects=True),
        cost_estimate=pl.CostEstimate(flops=1000, bytes_accessed=10**7, transcendentals=0),
        name="stats",
    )(mine)


def body(
    dec_hidden,
    enc_keys,
    enc_values,
    enc_lengths,
    cand_counts,
    gold_ids,
    gain_cross,
    w_query,
    w_out,
    gain_ffn,
    w_in_gate,
    w_in_up,
    w_ffn_out,
    gain_final,
    w_vocab,
):
    query_count, cand_dev, length_tok, model_width = dec_hidden.shape
    src_dev = enc_keys.shape[1]
    n = lax.axis_size("tok")
    nc = lax.axis_size("cand")
    tok_index = lax.axis_index("tok")
    j = lax.axis_index("cand")
    rows = query_count * cand_dev * length_tok
    per_query = cand_dev * length_tok
    share = rows // n
    head_cols = w_query.shape[1]
    heads_dev = head_cols // HEAD_DIM
    kc = model_width // nc

    def shifted(value, p):
        return lax.ppermute(value, "cand", [((i + p) % nc, i) for i in range(nc)])

    def ring(w):
        return [w] + [shifted(w, p) for p in range(1, nc)]

    def rotate(value, axis):
        size = value.shape[axis] // nc
        return jnp.concatenate(
            [
                lax.dynamic_slice_in_dim(value, ((j + p) % nc) * size, size, axis)
                for p in range(nc)
            ],
            axis,
        )

    wq, wo = ring(w_query), ring(w_out)
    wg, wu, wd = ring(w_in_gate), ring(w_in_up), ring(w_ffn_out)
    wv = ring(w_vocab)

    split = nc if heads_dev % nc == 0 else 1
    hc = head_cols // split
    hpd = hc // HEAD_DIM

    def pick(value):
        v = value.reshape(query_count, src_dev, n, split, hc)
        at = j if split > 1 else 0
        return lax.dynamic_index_in_dim(v, at, 3, keepdims=False)

    kv = jnp.concatenate([pick(enc_keys), pick(enc_values)], -1).transpose(2, 0, 1, 3)
    kv = lax.all_to_all(kv, "tok", split_axis=0, concat_axis=0, tiled=True)
    kv = kv.transpose(1, 0, 2, 3).reshape(query_count, n * src_dev, 2 * hc)
    keys = kv[..., :hc].reshape(query_count, -1, hpd, HEAD_DIM)
    values = kv[..., hc:].reshape(query_count, -1, hpd, HEAD_DIM)

    x_rot = rotate(dec_hidden.reshape(rows, model_width), 1)
    gain_cross, gain_ffn, gain_final = (
        rotate(g, 0) for g in (gain_cross, gain_ffn, gain_final)
    )
    normed = root_norm(x_rot.astype(F32), gain_cross).astype(BF)

    def deep(left_side, shards):
        total = dot32(left_side[:, :kc], shards[0])
        for p in range(1, nc):
            total = total + dot32(left_side[:, p * kc : (p + 1) * kc], shards[p])
        return total

    query_local = deep(normed, wq).astype(BF)
    if split > 1:
        groups = []
        for p in range(nc):
            cols = lax.dynamic_slice_in_dim(query_local, ((j + nc - p) % nc) * hc, hc, 1)
            groups.append(cols if p == 0 else shifted(cols, p))
        query = jnp.stack(groups)
    else:
        query = query_local[None]
    ng = query.shape[0]
    query = query.reshape(ng, query_count, per_query, hpd, HEAD_DIM)
    query = query.transpose(1, 0, 2, 3, 4).reshape(query_count, ng * per_query, hpd, HEAD_DIM)

    live = (lax.iota(jnp.int32, n * src_dev)[None, :] < enc_lengths[:, None])[:, None, None, :]
    scores = jnp.einsum("brhd,bshd->bhrs", query, keys, preferred_element_type=F32)
    scores = jnp.where(live, scores, -1e30)
    row_max = jnp.max(scores, axis=-1, keepdims=True)
    weights = jnp.where(live, jnp.exp(scores - row_max), 0.0)
    denominator = jnp.sum(weights, axis=-1)
    mixed = jnp.einsum(
        "bhrs,bshd->brhd", weights.astype(BF), values, preferred_element_type=F32
    )
    attended = (mixed / denominator.transpose(0, 2, 1)[..., None]).astype(BF)
    attended = attended.reshape(query_count, ng, per_query, hc).transpose(1, 0, 2, 3)
    attended = attended.reshape(ng, rows, hc)
    if split > 1:
        heads = [attended[0]] + [
            lax.ppermute(attended[p], "cand", [(i, (i + p) % nc) for i in range(nc)])
            for p in range(1, nc)
        ]
        attended = jnp.concatenate(
            [lax.select_n((j + nc - b) % nc, *heads) if nc > 2 else jnp.where(j == b, heads[0], heads[1]) for b in range(nc)],
            axis=1,
        )
    else:
        attended = attended[0]

    resid = lax.dynamic_slice_in_dim(x_rot, tok_index * share, share, 0).astype(F32)
    after_cross, ffn_every = mix([dot32(attended, w) for w in wo], resid, gain_ffn, n, 1)
    ffn_every = ffn_every.reshape(rows, model_width)
    gate_part = deep(ffn_every, wg)
    up_part = deep(ffn_every, wu)
    hidden = (jax.nn.gelu(gate_part, approximate=True) * up_part).astype(BF)
    _, final_every = mix([dot32(hidden, w) for w in wd], after_cross, gain_final, n, 2)
    final_every = final_every.reshape(rows, model_width)

    vocab_cols = w_vocab.shape[1]
    logits = deep(final_every, wv)
    gold_flat = gold_ids.reshape(rows)
    matches = (
        lax.iota(jnp.int32, vocab_cols)[None, :] == (gold_flat - tok_index * vocab_cols)[:, None]
    )
    gold_local = jnp.sum(jnp.where(matches, logits, 0.0), axis=1)
    local_max = jnp.max(logits, axis=1)
    local_sum = jnp.sum(jnp.exp(logits - local_max[:, None]), axis=1)
    stats = gather_stats(jnp.stack([local_max, local_sum, gold_local]).reshape(-1, 128), n)
    stats = stats.reshape(n, 3, rows)
    global_max = jnp.max(stats[:, 0], axis=0)
    sum_exp = jnp.sum(stats[:, 1] * jnp.exp(stats[:, 0] - global_max), axis=0)
    gold_logit = jnp.sum(stats[:, 2], axis=0)
    logprob = gold_logit - global_max - jnp.log(sum_exp)
    per_cand = jnp.mean(logprob.reshape(query_count, cand_dev, length_tok), axis=2)
    cand_index = j * cand_dev + lax.iota(jnp.int32, cand_dev)
    valid_cand = cand_index[None, :] < cand_counts[:, None]
    cand_scores = jnp.where(valid_cand, per_cand, 0.0)
    best_local = jnp.max(jnp.where(valid_cand, per_cand, -1e30), axis=1)
    best_score = lax.pmax(best_local, "cand")
    return (cand_scores, best_score)


def solution(mesh):
    in_specs = (
        P(None, "cand", None, None),
        P(None, "tok", None),
        P(None, "tok", None),
        P(),
        P(),
        P(None, "cand", None),
        P(),
        P("cand", "tok"),
        P("tok", "cand"),
        P(),
        P("cand", "tok"),
        P("cand", "tok"),
        P("tok", "cand"),
        P(),
        P("cand", "tok"),
    )
    out_specs = (P(None, "cand"), P())
    return jax.shard_map(body, mesh=mesh, in_specs=in_specs, out_specs=out_specs, check_vma=False)
```

```python
import functools

import jax
import jax.numpy as jnp
from jax import lax
from jax.experimental import pallas as pl
from jax.experimental.pallas import tpu as pltpu
from jax.sharding import PartitionSpec as P


HEAD_DIM = 64
MESH = pl.DeviceIdType.MESH

norm_eps = 0.25
BF = jnp.bfloat16
F32 = jnp.float32


def root_norm(values, gain):
    squares = jnp.mean(values * values, axis=-1, keepdims=True)
    return values * lax.rsqrt(squares + norm_eps) * gain


def dot32(left_side, piece):
    return jnp.dot(left_side, piece, preferred_element_type=F32)


def mix_kernel(n, pieces, sub, *refs):
    part = refs[:pieces]
    resid, gain = refs[pieces : pieces + 2]
    after, every = refs[pieces + 2 : pieces + 4]
    (
        send_c, recv_c, send_y, recv_y, send_z, recv_z,
        cs, cr, ys, yr, zs, zr, gzs, gzr, gys, gyr, gcs, gcr,
    ) = refs[pieces + 4 :]
    outer = n // 4
    width = send_c.shape[-1]
    chunks = pieces * sub
    me = lax.axis_index("tok")
    a, y, c = me // 4, (me // 2) % 2, me % 2
    core_peer = a * 4 + y * 2 + (1 - c)
    mid_peer = a * 4 + (1 - y) * 2 + c

    def outer_peer(k):
        return ((a + k) % outer) * 4 + y * 2 + c

    barrier = pltpu.get_barrier_semaphore()
    peers = [core_peer, mid_peer] + [outer_peer(k) for k in range(1, outer)]
    for peer in peers:
        pl.semaphore_signal(barrier, inc=1, device_id={"tok": peer}, device_id_type=MESH)

    def remote(src, dst, s, r, peer):
        return pltpu.make_async_remote_copy(
            src_ref=src, dst_ref=dst, send_sem=s, recv_sem=r,
            device_id={"tok": peer}, device_id_type=MESH,
        )

    def piece_of(ch):
        at = (ch % sub) * width
        return part[ch // sub], slice(at, at + width)

    copies = []
    for ch in range(chunks):
        ref, cols = piece_of(ch)
        for i in range(outer):
            for m in range(2):
                send_c[ch, i * 2 + m] = ref[i * 4 + m * 2 + (1 - c), :, cols].astype(BF)
        if ch == 0:
            pl.semaphore_wait(barrier, len(peers))
        cp = remote(send_c.at[ch], recv_c.at[ch], cs.at[ch], cr.at[ch], core_peer)
        cp.start()
        copies.append(cp)
    core_copies = list(copies)
    mid_copies = []
    for ch in range(chunks):
        ref, cols = piece_of(ch)
        core_copies[ch].wait_recv()
        for i in range(outer):
            other = 1 - y
            send_y[ch, i] = (
                ref[i * 4 + other * 2 + c, :, cols] + recv_c[ch, i * 2 + other].astype(F32)
            ).astype(BF)
        cp = remote(send_y.at[ch], recv_y.at[ch], ys.at[ch], yr.at[ch], mid_peer)
        cp.start()
        copies.append(cp)
        mid_copies.append(cp)

    def joined(ch, i):
        ref, cols = piece_of(ch)
        return (
            ref[i * 4 + y * 2 + c, :, cols]
            + recv_c[ch, i * 2 + y].astype(F32)
            + recv_y[ch, i].astype(F32)
        )

    outer_copies = []
    for ch in range(chunks):
        mid_copies[ch].wait_recv()
        row = []
        for k in range(1, outer):
            to = (a + k) % outer
            send_z[ch, k - 1] = joined(ch, to).astype(BF)
            cp = remote(
                send_z.at[ch, k - 1], recv_z.at[ch, k - 1],
                zs.at[ch, k - 1], zr.at[ch, k - 1], outer_peer(k),
            )
            cp.start()
            copies.append(cp)
            row.append(cp)
        outer_copies.append(row)
    for ch in range(chunks):
        total = joined(ch, a)
        for k in range(1, outer):
            outer_copies[ch][k - 1].wait_recv()
            total = total + recv_z[ch, k - 1].astype(F32)
        cols = slice(ch * width, (ch + 1) * width)
        after[:, cols] = resid[:, cols] + total
    values = after[...]
    every[me] = root_norm(values, gain[...]).astype(BF)

    gz, gy, gc = [], [], []
    for k in range(1, outer):
        cp = remote(every.at[me], every.at[me], gzs.at[k - 1], gzr.at[k - 1], outer_peer(k))
        cp.start()
        gz.append(cp)

    def block(k, m, e):
        return ((a + outer - k) % outer) * 4 + m * 2 + e

    def to_mid(k):
        b = block(k, y, c)
        cp = remote(every.at[b], every.at[b], gys.at[k], gyr.at[k], mid_peer)
        cp.start()
        gy.append(cp)

    def to_core(k, m, slot):
        b = block(k, m, c)
        cp = remote(every.at[b], every.at[b], gcs.at[slot], gcr.at[slot], core_peer)
        cp.start()
        gc.append(cp)

    to_mid(0)
    to_core(0, y, 0)
    for k in range(1, outer):
        gz[k - 1].wait_recv()
        to_mid(k)
        to_core(k, y, 2 * k)
    for k in range(outer):
        gy[k].wait_recv()
        to_core(k, 1 - y, 2 * k + 1)
    for cp in gc:
        cp.wait_recv()
    for cp in copies + gz + gy + gc:
        cp.wait_send()


def mix(parts, resid, gain, n, ident):
    pieces = len(parts)
    share, width = resid.shape
    sub = max(1, 4 // pieces)
    cw = width // pieces // sub
    chunks = pieces * sub
    outer = n // 4
    vm = pl.BlockSpec(memory_space=pltpu.VMEM)
    dma = pltpu.SemaphoreType.DMA
    parts = [p.reshape(n, share, width // pieces) for p in parts]
    return pl.pallas_call(
        functools.partial(mix_kernel, n, pieces, sub),
        out_shape=(
            jax.ShapeDtypeStruct((share, width), F32),
            jax.ShapeDtypeStruct((n, share, width), BF),
        ),
        in_specs=[vm] * (pieces + 2),
        out_specs=(vm, vm),
        scratch_shapes=[
            pltpu.VMEM((chunks, outer * 2, share, cw), BF),
            pltpu.VMEM((chunks, outer * 2, share, cw), BF),
            pltpu.VMEM((chunks, outer, share, cw), BF),
            pltpu.VMEM((chunks, outer, share, cw), BF),
            pltpu.VMEM((chunks, outer - 1, share, cw), BF),
            pltpu.VMEM((chunks, outer - 1, share, cw), BF),
            dma((chunks,)), dma((chunks,)), dma((chunks,)), dma((chunks,)),
            dma((chunks, outer - 1)), dma((chunks, outer - 1)),
            dma((outer - 1,)), dma((outer - 1,)),
            dma((outer,)), dma((outer,)), dma((2 * outer,)), dma((2 * outer,)),
        ],
        compiler_params=pltpu.CompilerParams(
            collective_id=ident, has_side_effects=True, vmem_limit_bytes=32 << 20
        ),
        cost_estimate=pl.CostEstimate(
            flops=10**7, bytes_accessed=100 * 10**6, transcendentals=0
        ),
    )(*parts, resid, gain.reshape(1, width))


def stats_kernel(n, mine, out, ss, rs):
    me = lax.axis_index("tok")
    barrier = pltpu.get_barrier_semaphore()
    for k in range(1, n):
        pl.semaphore_signal(
            barrier, inc=1, device_id={"tok": (me + k) % n}, device_id_type=MESH
        )
    out[me] = mine[...]
    pl.semaphore_wait(barrier, n - 1)
    copies = []
    for k in range(1, n):
        cp = pltpu.make_async_remote_copy(
            src_ref=mine, dst_ref=out.at[me], send_sem=ss.at[k - 1], recv_sem=rs.at[k - 1],
            device_id={"tok": (me + k) % n}, device_id_type=MESH,
        )
        cp.start()
        copies.append(cp)
    for cp in copies:
        cp.wait_recv()
    for cp in copies:
        cp.wait_send()


def gather_stats(mine, n):
    vm = pl.BlockSpec(memory_space=pltpu.VMEM)
    return pl.pallas_call(
        functools.partial(stats_kernel, n),
        out_shape=jax.ShapeDtypeStruct((n,) + mine.shape, F32),
        in_specs=[vm],
        out_specs=vm,
        scratch_shapes=[pltpu.SemaphoreType.DMA((n - 1,)), pltpu.SemaphoreType.DMA((n - 1,))],
        compiler_params=pltpu.CompilerParams(collective_id=3, has_side_effects=True),
        cost_estimate=pl.CostEstimate(flops=1000, bytes_accessed=10**7, transcendentals=0),
        name="stats",
    )(mine)


VOCAB_CHUNKS = 4


def body(
    dec_hidden,
    enc_keys,
    enc_values,
    enc_lengths,
    cand_counts,
    gold_ids,
    gain_cross,
    w_query,
    w_out,
    gain_ffn,
    w_in_gate,
    w_in_up,
    w_ffn_out,
    gain_final,
    w_vocab,
):
    query_count, cand_dev, length_tok, model_width = dec_hidden.shape
    src_dev = enc_keys.shape[1]
    n = lax.axis_size("tok")
    nc = lax.axis_size("cand")
    tok_index = lax.axis_index("tok")
    j = lax.axis_index("cand")
    rows = query_count * cand_dev * length_tok
    per_query = cand_dev * length_tok
    share = rows // n
    head_cols = w_query.shape[1]
    heads_dev = head_cols // HEAD_DIM
    kc = model_width // nc

    def shifted(value, p):
        return lax.ppermute(value, "cand", [((i + p) % nc, i) for i in range(nc)])

    def ring(w):
        return [w] + [shifted(w, p) for p in range(1, nc)]

    def rotate(value, axis):
        size = value.shape[axis] // nc
        return jnp.concatenate(
            [
                lax.dynamic_slice_in_dim(value, ((j + p) % nc) * size, size, axis)
                for p in range(nc)
            ],
            axis,
        )

    vocab_cols = w_vocab.shape[1]
    step = -(-vocab_cols // VOCAB_CHUNKS // 8) * 8
    edges = [min(i * step, vocab_cols) for i in range(VOCAB_CHUNKS + 1)]
    wq, wo = ring(w_query), ring(w_out)
    wg, wu, wd = ring(w_in_gate), ring(w_in_up), ring(w_ffn_out)
    wv = [ring(w_vocab[:, lo:hi]) for lo, hi in zip(edges, edges[1:])]

    split = nc if heads_dev % nc == 0 else 1
    hc = head_cols // split
    hpd = hc // HEAD_DIM

    def pick(value):
        v = value.reshape(query_count, src_dev, n, split, hc)
        at = j if split > 1 else 0
        return lax.dynamic_index_in_dim(v, at, 3, keepdims=False)

    kv = jnp.concatenate([pick(enc_keys), pick(enc_values)], -1).transpose(2, 0, 1, 3)
    kv = lax.all_to_all(kv, "tok", split_axis=0, concat_axis=0, tiled=True)
    kv = kv.transpose(1, 0, 2, 3).reshape(query_count, n * src_dev, 2 * hc)
    keys = kv[..., :hc].reshape(query_count, -1, hpd, HEAD_DIM)
    values = kv[..., hc:].reshape(query_count, -1, hpd, HEAD_DIM)

    x_rot = rotate(dec_hidden.reshape(rows, model_width), 1)
    gain_cross, gain_ffn, gain_final = (
        rotate(g, 0) for g in (gain_cross, gain_ffn, gain_final)
    )
    normed = root_norm(x_rot.astype(F32), gain_cross).astype(BF)

    def deep(left_side, shards):
        total = dot32(left_side[:, :kc], shards[0])
        for p in range(1, nc):
            total = total + dot32(left_side[:, p * kc : (p + 1) * kc], shards[p])
        return total

    query_local = deep(normed, wq).astype(BF)
    if split > 1:
        groups = []
        for p in range(nc):
            cols = lax.dynamic_slice_in_dim(query_local, ((j + nc - p) % nc) * hc, hc, 1)
            groups.append(cols if p == 0 else shifted(cols, p))
        query = jnp.stack(groups)
    else:
        query = query_local[None]
    ng = query.shape[0]
    query = query.reshape(ng, query_count, per_query, hpd, HEAD_DIM)
    query = query.transpose(1, 0, 2, 3, 4).reshape(query_count, ng * per_query, hpd, HEAD_DIM)

    live = (lax.iota(jnp.int32, n * src_dev)[None, :] < enc_lengths[:, None])[:, None, None, :]
    scores = jnp.einsum("brhd,bshd->bhrs", query, keys, preferred_element_type=F32)
    scores = jnp.where(live, scores, -1e30)
    row_max = jnp.max(scores, axis=-1, keepdims=True)
    weights = jnp.where(live, jnp.exp(scores - row_max), 0.0)
    denominator = jnp.sum(weights, axis=-1)
    mixed = jnp.einsum(
        "bhrs,bshd->brhd", weights.astype(BF), values, preferred_element_type=F32
    )
    attended = (mixed / denominator.transpose(0, 2, 1)[..., None]).astype(BF)
    attended = attended.reshape(query_count, ng, per_query, hc).transpose(1, 0, 2, 3)
    attended = attended.reshape(ng, rows, hc)
    if split > 1:
        heads = [attended[0]] + [
            lax.ppermute(attended[p], "cand", [(i, (i + p) % nc) for i in range(nc)])
            for p in range(1, nc)
        ]
        attended = jnp.concatenate(
            [lax.select_n((j + nc - b) % nc, *heads) if nc > 2 else jnp.where(j == b, heads[0], heads[1]) for b in range(nc)],
            axis=1,
        )
    else:
        attended = attended[0]

    resid = lax.dynamic_slice_in_dim(x_rot, tok_index * share, share, 0).astype(F32)
    after_cross, ffn_every = mix([dot32(attended, w) for w in wo], resid, gain_ffn, n, 1)
    ffn_every = ffn_every.reshape(rows, model_width)
    gate_part = deep(ffn_every, wg)
    up_part = deep(ffn_every, wu)
    hidden = (jax.nn.gelu(gate_part, approximate=True) * up_part).astype(BF)
    _, final_every = mix([dot32(hidden, w) for w in wd], after_cross, gain_final, n, 2)
    final_every = final_every.reshape(rows, model_width)

    gold_here = gold_ids.reshape(rows) - tok_index * vocab_cols
    maxima, sums, golds = [], [], []
    for lo, hi, shards in zip(edges, edges[1:], wv):
        logits = deep(final_every, shards)
        matches = lo + lax.iota(jnp.int32, hi - lo)[None, :] == gold_here[:, None]
        golds.append(jnp.sum(jnp.where(matches, logits, 0.0), axis=1))
        maxima.append(jnp.max(logits, axis=1))
        sums.append(jnp.sum(jnp.exp(logits - maxima[-1][:, None]), axis=1))
    local_max = functools.reduce(jnp.maximum, maxima)
    local_sum = sum(t * jnp.exp(m - local_max) for t, m in zip(sums, maxima))
    gold_local = sum(golds)
    stats = gather_stats(jnp.stack([local_max, local_sum, gold_local]).reshape(-1, 128), n)
    stats = stats.reshape(n, 3, rows)
    global_max = jnp.max(stats[:, 0], axis=0)
    sum_exp = jnp.sum(stats[:, 1] * jnp.exp(stats[:, 0] - global_max), axis=0)
    gold_logit = jnp.sum(stats[:, 2], axis=0)
    logprob = gold_logit - global_max - jnp.log(sum_exp)
    per_cand = jnp.mean(logprob.reshape(query_count, cand_dev, length_tok), axis=2)
    cand_index = j * cand_dev + lax.iota(jnp.int32, cand_dev)
    valid_cand = cand_index[None, :] < cand_counts[:, None]
    cand_scores = jnp.where(valid_cand, per_cand, 0.0)
    best_local = jnp.max(jnp.where(valid_cand, per_cand, -1e30), axis=1)
    best_score = lax.pmax(best_local, "cand")
    return (cand_scores, best_score)


def solution(mesh):
    in_specs = (
        P(None, "cand", None, None),
        P(None, "tok", None),
        P(None, "tok", None),
        P(),
        P(),
        P(None, "cand", None),
        P(),
        P("cand", "tok"),
        P("tok", "cand"),
        P(),
        P("cand", "tok"),
        P("cand", "tok"),
        P("tok", "cand"),
        P(),
        P("cand", "tok"),
    )
    out_specs = (P(None, "cand"), P())

    return jax.shard_map(body, mesh=mesh, in_specs=in_specs, out_specs=out_specs, check_vma=False)
```

```python
import functools

import jax
import jax.numpy as jnp
from jax import lax
from jax.experimental import pallas as pl
from jax.experimental.pallas import tpu as pltpu
from jax.sharding import PartitionSpec as P


HEAD_DIM = 64
MESH = pl.DeviceIdType.MESH

norm_eps = 0.25
BF = jnp.bfloat16
F32 = jnp.float32


def root_norm(values, gain):
    squares = jnp.mean(values * values, axis=-1, keepdims=True)
    return values * lax.rsqrt(squares + norm_eps) * gain


def dot32(left_side, piece):
    return jnp.dot(left_side, piece, preferred_element_type=F32)


def mix_kernel(n, pieces, sub, *refs):
    part = refs[:pieces]
    resid, gain = refs[pieces : pieces + 2]
    after, every = refs[pieces + 2 : pieces + 4]
    (
        send_c, recv_c, send_y, recv_y, send_z, recv_z,
        cs, cr, ys, yr, zs, zr, gzs, gzr, gys, gyr, gcs, gcr,
    ) = refs[pieces + 4 :]
    outer = n // 4
    width = send_c.shape[-1]
    chunks = pieces * sub
    me = lax.axis_index("tok")
    a, y, c = me // 4, (me // 2) % 2, me % 2
    core_peer = a * 4 + y * 2 + (1 - c)
    mid_peer = a * 4 + (1 - y) * 2 + c

    def outer_peer(k):
        return ((a + k) % outer) * 4 + y * 2 + c

    barrier = pltpu.get_barrier_semaphore()
    peers = [core_peer, mid_peer] + [outer_peer(k) for k in range(1, outer)]
    for peer in peers:
        pl.semaphore_signal(barrier, inc=1, device_id={"tok": peer}, device_id_type=MESH)

    def remote(src, dst, s, r, peer):
        return pltpu.make_async_remote_copy(
            src_ref=src, dst_ref=dst, send_sem=s, recv_sem=r,
            device_id={"tok": peer}, device_id_type=MESH,
        )

    def piece_of(ch):
        at = (ch % sub) * width
        return part[ch // sub], slice(at, at + width)

    copies = []
    for ch in range(chunks):
        ref, cols = piece_of(ch)
        for i in range(outer):
            for m in range(2):
                send_c[ch, i * 2 + m] = ref[i * 4 + m * 2 + (1 - c), :, cols].astype(BF)
        if ch == 0:
            pl.semaphore_wait(barrier, len(peers))
        cp = remote(send_c.at[ch], recv_c.at[ch], cs.at[ch], cr.at[ch], core_peer)
        cp.start()
        copies.append(cp)
    core_copies = list(copies)
    mid_copies = []
    for ch in range(chunks):
        ref, cols = piece_of(ch)
        core_copies[ch].wait_recv()
        for i in range(outer):
            other = 1 - y
            send_y[ch, i] = (
                ref[i * 4 + other * 2 + c, :, cols] + recv_c[ch, i * 2 + other].astype(F32)
            ).astype(BF)
        cp = remote(send_y.at[ch], recv_y.at[ch], ys.at[ch], yr.at[ch], mid_peer)
        cp.start()
        copies.append(cp)
        mid_copies.append(cp)

    def joined(ch, i):
        ref, cols = piece_of(ch)
        return (
            ref[i * 4 + y * 2 + c, :, cols]
            + recv_c[ch, i * 2 + y].astype(F32)
            + recv_y[ch, i].astype(F32)
        )

    outer_copies = []
    for ch in range(chunks):
        mid_copies[ch].wait_recv()
        row = []
        for k in range(1, outer):
            to = (a + k) % outer
            send_z[ch, k - 1] = joined(ch, to).astype(BF)
            cp = remote(
                send_z.at[ch, k - 1], recv_z.at[ch, k - 1],
                zs.at[ch, k - 1], zr.at[ch, k - 1], outer_peer(k),
            )
            cp.start()
            copies.append(cp)
            row.append(cp)
        outer_copies.append(row)
    for ch in range(chunks):
        total = joined(ch, a)
        for k in range(1, outer):
            outer_copies[ch][k - 1].wait_recv()
            total = total + recv_z[ch, k - 1].astype(F32)
        cols = slice(ch * width, (ch + 1) * width)
        after[:, cols] = resid[:, cols] + total
    values = after[...]
    every[me] = root_norm(values, gain[...]).astype(BF)

    gz, gy, gc = [], [], []
    for k in range(1, outer):
        cp = remote(every.at[me], every.at[me], gzs.at[k - 1], gzr.at[k - 1], outer_peer(k))
        cp.start()
        gz.append(cp)

    def block(k, m, e):
        return ((a + outer - k) % outer) * 4 + m * 2 + e

    def to_mid(k):
        b = block(k, y, c)
        cp = remote(every.at[b], every.at[b], gys.at[k], gyr.at[k], mid_peer)
        cp.start()
        gy.append(cp)

    def to_core(k, m, slot):
        b = block(k, m, c)
        cp = remote(every.at[b], every.at[b], gcs.at[slot], gcr.at[slot], core_peer)
        cp.start()
        gc.append(cp)

    to_mid(0)
    to_core(0, y, 0)
    for k in range(1, outer):
        gz[k - 1].wait_recv()
        to_mid(k)
        to_core(k, y, 2 * k)
    for k in range(outer):
        gy[k].wait_recv()
        to_core(k, 1 - y, 2 * k + 1)
    for cp in gc:
        cp.wait_recv()
    for cp in copies + gz + gy + gc:
        cp.wait_send()


def mix(parts, resid, gain, n, ident):
    pieces = len(parts)
    share, width = resid.shape
    sub = max(1, 4 // pieces)
    cw = width // pieces // sub
    chunks = pieces * sub
    outer = n // 4
    vm = pl.BlockSpec(memory_space=pltpu.VMEM)
    dma = pltpu.SemaphoreType.DMA
    parts = [p.reshape(n, share, width // pieces) for p in parts]
    return pl.pallas_call(
        functools.partial(mix_kernel, n, pieces, sub),
        out_shape=(
            jax.ShapeDtypeStruct((share, width), F32),
            jax.ShapeDtypeStruct((n, share, width), BF),
        ),
        in_specs=[vm] * (pieces + 2),
        out_specs=(vm, vm),
        scratch_shapes=[
            pltpu.VMEM((chunks, outer * 2, share, cw), BF),
            pltpu.VMEM((chunks, outer * 2, share, cw), BF),
            pltpu.VMEM((chunks, outer, share, cw), BF),
            pltpu.VMEM((chunks, outer, share, cw), BF),
            pltpu.VMEM((chunks, outer - 1, share, cw), BF),
            pltpu.VMEM((chunks, outer - 1, share, cw), BF),
            dma((chunks,)), dma((chunks,)), dma((chunks,)), dma((chunks,)),
            dma((chunks, outer - 1)), dma((chunks, outer - 1)),
            dma((outer - 1,)), dma((outer - 1,)),
            dma((outer,)), dma((outer,)), dma((2 * outer,)), dma((2 * outer,)),
        ],
        compiler_params=pltpu.CompilerParams(
            collective_id=ident, has_side_effects=True, vmem_limit_bytes=32 << 20
        ),
        cost_estimate=pl.CostEstimate(
            flops=10**7, bytes_accessed=100 * 10**6, transcendentals=0
        ),
    )(*parts, resid, gain.reshape(1, width))


def score_kernel(n, nc, per, length, counts, mine, out, best, got, best_got, ss, rs, bs, br):
    me, j = lax.axis_index("tok"), lax.axis_index("cand")
    barrier = pltpu.get_barrier_semaphore()
    for k in range(1, n):
        pl.semaphore_signal(
            barrier, inc=1, device_id={"tok": (me + k) % n}, device_id_type=MESH
        )
    for p in range(1, nc):
        pl.semaphore_signal(
            barrier, inc=1, device_id={"cand": (j + p) % nc}, device_id_type=MESH
        )
    got[me] = mine[...]
    pl.semaphore_wait(barrier, n + nc - 2)
    copies = []
    for k in range(1, n):
        cp = pltpu.make_async_remote_copy(
            src_ref=mine, dst_ref=got.at[me], send_sem=ss.at[k - 1], recv_sem=rs.at[k - 1],
            device_id={"tok": (me + k) % n}, device_id_type=MESH,
        )
        cp.start()
        copies.append(cp)
    for cp in copies:
        cp.wait_recv()
    lines = mine.shape[0] // 2
    every = got[...]
    parts = every[:, :lines]
    top = jnp.max(parts, axis=0)
    total = top + jnp.log(jnp.sum(jnp.exp(parts - top), axis=0))
    logprob = jnp.sum(every[:, lines:], axis=0) - total
    per_line = 128 // length
    group = lax.broadcasted_iota(jnp.int32, (lines, 128), 1) // length
    line = lax.broadcasted_iota(jnp.int32, (lines, 128), 0)
    mean = jnp.zeros((lines, 128), F32)
    for g in range(per_line):
        held = group == g
        value = jnp.sum(jnp.where(held, logprob, 0.0), axis=1, keepdims=True) / length
        mean = jnp.where(held, value, mean)
    which = line * per_line + group
    place = j * per + which % per
    owner = which // per
    queries = lines * per_line // per
    row = lax.broadcasted_iota(jnp.int32, (8, 128), 0)
    tops = jnp.full((8, 128), -1e30, F32)
    scores = jnp.zeros((lines, 128), F32)
    for b in range(queries):
        valid = (owner == b) & (place < counts[b])
        scores = jnp.where(valid, mean, scores)
        high = jnp.max(jnp.where(valid, mean, -1e30), axis=(0, 1), keepdims=True)
        tops = jnp.where(row == b, high, tops)
    out[...] = scores
    best_got[j] = tops
    more = []
    for p in range(1, nc):
        cp = pltpu.make_async_remote_copy(
            src_ref=best_got.at[j], dst_ref=best_got.at[j],
            send_sem=bs.at[p - 1], recv_sem=br.at[p - 1],
            device_id={"cand": (j + p) % nc}, device_id_type=MESH,
        )
        cp.start()
        more.append(cp)
    for cp in more:
        cp.wait_recv()
    best[...] = jnp.max(best_got[...], axis=0)
    for cp in copies + more:
        cp.wait_send()


def final_scores(mine, counts, n, nc, per, length):
    vm = pl.BlockSpec(memory_space=pltpu.VMEM)
    dma = pltpu.SemaphoreType.DMA
    return pl.pallas_call(
        functools.partial(score_kernel, n, nc, per, length),
        out_shape=(
            jax.ShapeDtypeStruct((mine.shape[0] // 2, 128), F32),
            jax.ShapeDtypeStruct((8, 128), F32),
        ),
        in_specs=[pl.BlockSpec(memory_space=pltpu.SMEM), vm],
        out_specs=(vm, vm),
        scratch_shapes=[
            pltpu.VMEM((n,) + mine.shape, F32),
            pltpu.VMEM((nc, 8, 128), F32),
            dma((n - 1,)), dma((n - 1,)), dma((nc - 1,)), dma((nc - 1,)),
        ],
        compiler_params=pltpu.CompilerParams(collective_id=3, has_side_effects=True),
        cost_estimate=pl.CostEstimate(flops=1000, bytes_accessed=10**7, transcendentals=0),
        name="score",
    )(counts, mine)


VOCAB_CHUNKS = 4


def body(
    dec_hidden,
    enc_keys,
    enc_values,
    enc_lengths,
    cand_counts,
    gold_ids,
    gain_cross,
    w_query,
    w_out,
    gain_ffn,
    w_in_gate,
    w_in_up,
    w_ffn_out,
    gain_final,
    w_vocab,
):
    query_count, cand_dev, length_tok, model_width = dec_hidden.shape
    src_dev = enc_keys.shape[1]
    n = lax.axis_size("tok")
    nc = lax.axis_size("cand")
    tok_index = lax.axis_index("tok")
    j = lax.axis_index("cand")
    rows = query_count * cand_dev * length_tok
    per_query = cand_dev * length_tok
    share = rows // n
    head_cols = w_query.shape[1]
    heads_dev = head_cols // HEAD_DIM
    kc = model_width // nc

    def shifted(value, p):
        return lax.ppermute(value, "cand", [((i + p) % nc, i) for i in range(nc)])

    def ring(w):
        return [w] + [shifted(w, p) for p in range(1, nc)]

    def rotate(value, axis):
        size = value.shape[axis] // nc
        return jnp.concatenate(
            [
                lax.dynamic_slice_in_dim(value, ((j + p) % nc) * size, size, axis)
                for p in range(nc)
            ],
            axis,
        )

    vocab_cols = w_vocab.shape[1]
    step = -(-vocab_cols // VOCAB_CHUNKS // 8) * 8
    edges = [min(i * step, vocab_cols) for i in range(VOCAB_CHUNKS + 1)]
    wq, wo = ring(w_query), ring(w_out)
    wg, wu, wd = ring(w_in_gate), ring(w_in_up), ring(w_ffn_out)
    wv = [ring(w_vocab[:, lo:hi]) for lo, hi in zip(edges, edges[1:])]

    split = nc if heads_dev % nc == 0 else 1
    hc = head_cols // split
    hpd = hc // HEAD_DIM

    def pick(value):
        v = value.reshape(query_count, src_dev, n, split, hc)
        at = j if split > 1 else 0
        return lax.dynamic_index_in_dim(v, at, 3, keepdims=False)

    kv = jnp.concatenate([pick(enc_keys), pick(enc_values)], -1).transpose(2, 0, 1, 3)
    kv = lax.all_to_all(kv, "tok", split_axis=0, concat_axis=0, tiled=True)
    kv = kv.transpose(1, 0, 2, 3).reshape(query_count, n * src_dev, 2 * hc)
    keys = kv[..., :hc].reshape(query_count, -1, hpd, HEAD_DIM)
    values = kv[..., hc:].reshape(query_count, -1, hpd, HEAD_DIM)

    x_rot = rotate(dec_hidden.reshape(rows, model_width), 1)
    gain_cross, gain_ffn, gain_final = (
        rotate(g, 0) for g in (gain_cross, gain_ffn, gain_final)
    )
    normed = root_norm(x_rot.astype(F32), gain_cross).astype(BF)

    def deep(left_side, shards):
        total = dot32(left_side[:, :kc], shards[0])
        for p in range(1, nc):
            total = total + dot32(left_side[:, p * kc : (p + 1) * kc], shards[p])
        return total

    query_local = deep(normed, wq).astype(BF)
    if split > 1:
        groups = []
        for p in range(nc):
            cols = lax.dynamic_slice_in_dim(query_local, ((j + nc - p) % nc) * hc, hc, 1)
            groups.append(cols if p == 0 else shifted(cols, p))
        query = jnp.stack(groups)
    else:
        query = query_local[None]
    ng = query.shape[0]
    query = query.reshape(ng, query_count, per_query, hpd, HEAD_DIM)
    query = query.transpose(1, 0, 2, 3, 4).reshape(query_count, ng * per_query, hpd, HEAD_DIM)

    live = (lax.iota(jnp.int32, n * src_dev)[None, :] < enc_lengths[:, None])[:, None, None, :]
    scores = jnp.einsum("brhd,bshd->bhrs", query, keys, preferred_element_type=F32)
    scores = jnp.where(live, scores, -1e30)
    row_max = jnp.max(scores, axis=-1, keepdims=True)
    weights = jnp.where(live, jnp.exp(scores - row_max), 0.0)
    denominator = jnp.sum(weights, axis=-1)
    mixed = jnp.einsum(
        "bhrs,bshd->brhd", weights.astype(BF), values, preferred_element_type=F32
    )
    attended = (mixed / denominator.transpose(0, 2, 1)[..., None]).astype(BF)
    attended = attended.reshape(query_count, ng, per_query, hc).transpose(1, 0, 2, 3)
    attended = attended.reshape(ng, rows, hc)
    if split > 1:
        heads = [attended[0]] + [
            lax.ppermute(attended[p], "cand", [(i, (i + p) % nc) for i in range(nc)])
            for p in range(1, nc)
        ]
        attended = jnp.concatenate(
            [lax.select_n((j + nc - b) % nc, *heads) if nc > 2 else jnp.where(j == b, heads[0], heads[1]) for b in range(nc)],
            axis=1,
        )
    else:
        attended = attended[0]

    resid = lax.dynamic_slice_in_dim(x_rot, tok_index * share, share, 0).astype(F32)
    after_cross, ffn_every = mix([dot32(attended, w) for w in wo], resid, gain_ffn, n, 1)
    ffn_every = ffn_every.reshape(rows, model_width)
    gate_part = deep(ffn_every, wg)
    up_part = deep(ffn_every, wu)
    hidden = (jax.nn.gelu(gate_part, approximate=True) * up_part).astype(BF)
    _, final_every = mix([dot32(hidden, w) for w in wd], after_cross, gain_final, n, 2)
    final_every = final_every.reshape(rows, model_width)

    gold_here = gold_ids.reshape(rows) - tok_index * vocab_cols
    maxima, sums, golds = [], [], []
    for lo, hi, shards in zip(edges, edges[1:], wv):
        logits = deep(final_every, shards)
        matches = lo + lax.iota(jnp.int32, hi - lo)[None, :] == gold_here[:, None]
        golds.append(jnp.sum(jnp.where(matches, logits, 0.0), axis=1))
        maxima.append(jnp.max(logits, axis=1))
        sums.append(jnp.sum(jnp.exp(logits - maxima[-1][:, None]), axis=1))
    local_max = functools.reduce(jnp.maximum, maxima)
    local_sum = sum(t * jnp.exp(m - local_max) for t, m in zip(sums, maxima))
    gold_local = sum(golds)
    lse_local = local_max + jnp.log(local_sum)
    scores_all, best_all = final_scores(
        jnp.stack([lse_local, gold_local]).reshape(-1, 128), cand_counts, n, nc, cand_dev, length_tok
    )
    cand_scores = scores_all.reshape(query_count, cand_dev, length_tok)[:, :, 0]
    best_score = best_all[:query_count, 0]
    return (cand_scores, best_score)


def solution(mesh):
    in_specs = (
        P(None, "cand", None, None),
        P(None, "tok", None),
        P(None, "tok", None),
        P(),
        P(),
        P(None, "cand", None),
        P(),
        P("cand", "tok"),
        P("tok", "cand"),
        P(),
        P("cand", "tok"),
        P("cand", "tok"),
        P("tok", "cand"),
        P(),
        P("cand", "tok"),
    )
    out_specs = (P(None, "cand"), P())

    return jax.shard_map(body, mesh=mesh, in_specs=in_specs, out_specs=out_specs, check_vma=False)
```
